32 devices in a mesh: gx: 2 (over x), gy: 16 (over z, y, core).
Axes of the slice: x: 2, y: 2, z: 4, core: 2. Of those that a mesh axis runs over, the one named last changes fastest.
Arguments:
- right_side: float32 [262144], P(('gx', 'gy')), may hold values from -60 to 60
- reaction: float32 [262144], P(('gx', 'gy')), may hold values from 0.5 to 2
- cell_slots: int32 [125, 4096], P(None, ('gx', 'gy')), may hold values from 0 to 12543
- cell_level: int32 [4096], P(('gx', 'gy')), may hold values from 0 to 2
- con_masters: int32 [5, 8192], P(None, ('gx', 'gy')), may hold values from 0 to 12287
- con_rows: int32 [8192], P(('gx', 'gy')), may hold values from 0 to 9
- send_lists: int32 [8, 16384], P(None, ('gx', 'gy')), may hold values from 0 to 8191
Outputs:
- solution: float32 [262144], P(('gx', 'gy'))
- residual: float32 [262144], P(('gx', 'gy'))
The draws below stay inside these ranges and needn't reach their ends.
Inputs may be any that keep to these rules, and one draw needn't show every extreme that they name: `cell_slots`: column block of rank d indexes d's local list: its 8192 owned unknowns, then 512 values from each of ranks d - 1, ..., d - 4, then from d + 1, ..., d + 4, then its 256 constrained values (rank d = 16 gx + gy). `cell_level`: A cell of level l has side 2^(-l). `con_masters`: slots among the same rank's owned and ghost values. `con_rows`: row of the interpolation table: 5 fine nodes on each half of a coarse edge. `send_lists`: row j of rank s lists s's owned unknowns that fill ghost block j of rank s + j + 1 (j < 4) or of rank s - (j - 3); rows without such a rank are unused.
All inputs are finite; a program needn't handle non-finite values.
Results may differ from the reference program's by a relative error of at most 0.0002.
Values sent between devices are 32-bit elements; how exact they have to be, the bound alone decides.
A program may use at most 64 MiB of HBM per device.

```python
import math
import jax
import jax.numpy as jnp
import numpy as np
from jax import lax

NODES = 5
PEERS = 4
ITERS = 3
CELLS_DEV = 128
NOWN = 8192
GHOSTS = 512
NCON = 256
CELLS = 4096
NDOF = 262144
NCON_ALL = 8192
LISTS = 16384
N_GX = 2
N_GY = 16


def draw_right_side(key, part):
    entries = NDOF
    position = jnp.arange(entries, dtype=jnp.float32) / entries
    rising = 1.0 + 2.0 * position
    first_key = jax.random.fold_in(jax.random.fold_in(key, 11), 0)
    normal_part = jnp.clip(jax.random.normal(first_key, (entries,), jnp.float32), -4.0, 4.0)
    return (normal_part * rising).astype(jnp.float32)


def set_ends(drawn, own_key, low, largest):
    extent = drawn.shape
    spot = [jax.random.randint(jax.random.fold_in(own_key, axis), (), 0, extent[axis]) for axis in range(len(extent))]
    drawn = drawn.at[tuple(spot)].set(low)
    longest = extent.index(max(extent))
    spot[longest] = (spot[longest] + 1) % extent[longest]
    return drawn.at[tuple(spot)].set(largest)


def block_levels(stream_key, shape, cuts, smallest, largest):
    def one(dim, shards_of):
        steps = jax.random.uniform(jax.random.fold_in(jax.random.fold_in(stream_key, 6), dim), (shards_of,), jnp.float32, smallest / len(cuts), largest / len(cuts))
        return jnp.repeat(jnp.exp(steps), shape[dim] // shards_of).reshape((-1,) + (1,) * (len(shape) - dim - 1))

    gain = one(*cuts[0])
    for cut in cuts[1:]:
        gain = gain * one(*cut)
    return gain


def setup_inputs(seed: int = 0) -> dict:
    key_list = jax.random.split(jax.random.key(seed), 8)
    return {
        "right_side": draw_right_side(jax.random.fold_in(key_list[7], 71), 0),
        "reaction": jnp.clip(jnp.exp(math.log(2.0) - 1.3862944 * jax.random.uniform(key_list[1], (NDOF,), jnp.float32) ** block_levels(key_list[1], (NDOF,), ((0, 32),), -0.2, 0.2)), 0.5, 2.0),
        "cell_slots": set_ends(jax.random.randint(key_list[2], (NODES ** 3, CELLS), 0, NOWN + 2 * PEERS * GHOSTS + NCON), jax.random.fold_in(key_list[2], 1), 0, (NOWN + 2 * PEERS * GHOSTS + NCON) - 1).astype(jnp.int32),
        "cell_level": set_ends(jax.random.randint(key_list[3], (CELLS,), 0, 3), jax.random.fold_in(key_list[3], 1), 0, 2).astype(jnp.int32),
        "con_masters": set_ends(jax.random.randint(key_list[4], (NODES, NCON_ALL), 0, NOWN + 2 * PEERS * GHOSTS), jax.random.fold_in(key_list[4], 1), 0, (NOWN + 2 * PEERS * GHOSTS) - 1).astype(jnp.int32),
        "con_rows": set_ends(jax.random.randint(key_list[5], (NCON_ALL,), 0, 10), jax.random.fold_in(key_list[5], 1), 0, 9).astype(jnp.int32),
        "send_lists": set_ends(jax.random.randint(key_list[6], (2 * PEERS, LISTS), 0, NOWN), jax.random.fold_in(key_list[6], 1), 0, NOWN - 1).astype(jnp.int32),
    }


def lagrange(node_list, points):
    node_count = len(node_list)
    values = np.ones((len(points), node_count))
    derivs = np.zeros((len(points), node_count))
    for basis_node in range(node_count):
        for other_node in range(node_count):
            if other_node != basis_node:
                values[:, basis_node] = values[:, basis_node] * (points - node_list[other_node]) / (node_list[basis_node] - node_list[other_node])
        for skipped in range(node_count):
            if skipped != basis_node:
                product_term = np.ones(len(points)) / (node_list[basis_node] - node_list[skipped])
                for other_node in range(node_count):
                    if other_node != basis_node and other_node != skipped:
                        product_term = product_term * (points - node_list[other_node]) / (node_list[basis_node] - node_list[other_node])
                derivs[:, basis_node] = derivs[:, basis_node] + product_term
    return (values, derivs)

def tables():
    gll_offset = np.sqrt(3.0 / 7.0)
    lobatto = np.array([0.0, (1.0 - gll_offset) / 2.0, 0.5, (1.0 + gll_offset) / 2.0, 1.0])
    inner_point = np.sqrt(5.0 - 2.0 * np.sqrt(10.0 / 7.0)) / 3.0
    outer_point = np.sqrt(5.0 + 2.0 * np.sqrt(10.0 / 7.0)) / 3.0
    inner_weight = (322.0 + 13.0 * np.sqrt(70.0)) / 900.0
    outer_weight = (322.0 - 13.0 * np.sqrt(70.0)) / 900.0
    points = np.array([-outer_point, -inner_point, 0.0, inner_point, outer_point])
    gauss_weights = np.array([outer_weight, inner_weight, 128.0 / 225.0, inner_weight, outer_weight])
    points = (points + 1.0) / 2.0
    gauss_weights = gauss_weights / 2.0
    shapes, slopes = lagrange(lobatto, points)
    fine_points = np.concatenate([lobatto / 2.0, (1.0 + lobatto) / 2.0])
    interp, unused_slopes = lagrange(lobatto, fine_points)
    quad_weights = np.kron(gauss_weights, np.kron(gauss_weights, gauss_weights))
    grad_x = np.kron(slopes, np.kron(shapes, shapes))
    grad_y = np.kron(shapes, np.kron(slopes, shapes))
    grad_z = np.kron(shapes, np.kron(shapes, slopes))
    stiffness = np.zeros((125, 125))
    for gradient in (grad_x, grad_y, grad_z):
        stiffness = stiffness + gradient.T @ (quad_weights[:, None] * gradient)
    return (jnp.asarray(interp, jnp.float32), jnp.asarray(stiffness, jnp.float32))

def cell_laplace(cell_values, cell_scale, stiffness):
    product = jnp.dot(stiffness, cell_values, precision=lax.Precision.HIGHEST, preferred_element_type=jnp.float32)
    return product * cell_scale[None, :]

def local_apply(own_values, ghosts, slot_map, cell_scale, masters, weights, stiffness):
    local_list = jnp.concatenate([own_values, ghosts.reshape(-1)])
    picked = local_list[masters]
    resolved = lax.optimization_barrier(jnp.sum(weights * picked, axis=0))
    full_list = jnp.concatenate([local_list, resolved])
    cell_values = full_list[slot_map]
    contrib = cell_laplace(cell_values, cell_scale, stiffness)
    summed = jnp.zeros(full_list.shape, jnp.float32).at[slot_map.reshape(-1)].add(contrib.reshape(-1))
    split_at = local_list.shape[0]
    spread = summed[:split_at].at[masters.reshape(-1)].add((weights * summed[split_at:][None, :]).reshape(-1))
    return spread

def reference(right_side, reaction, cell_slots, cell_level, con_masters, con_rows, send_lists):
    interp, stiffness = tables()
    rank_count = N_GX * N_GY
    block_count = 2 * PEERS
    offsets = [neighbour + 1 for neighbour in range(PEERS)] + [-(neighbour + 1) for neighbour in range(PEERS)]
    slot_maps = cell_slots.reshape(125, rank_count, CELLS_DEV).transpose(1, 0, 2)
    scales = jnp.exp2(-cell_level.astype(jnp.float32)).reshape(rank_count, CELLS_DEV)
    master_maps = con_masters.reshape(5, rank_count, NCON).transpose(1, 0, 2)
    selector = (con_rows.reshape(rank_count, NCON)[:, None, :] == jnp.arange(10, dtype=jnp.int32)[None, :, None]).astype(jnp.float32)
    weight_maps = jnp.einsum('tk,rtn->rkn', interp, selector, precision=lax.Precision.HIGHEST)
    list_rows = send_lists.reshape(block_count, rank_count, GHOSTS).transpose(1, 0, 2)
    rank_ids = jnp.arange(rank_count, dtype=jnp.int32)
    reactions = reaction.reshape(rank_count, NOWN)
    source_ids = [rank_ids - offset for offset in offsets]
    inside = [(source >= 0) & (source < rank_count) for source in source_ids]
    owner_ids = [jnp.clip(source, 0, rank_count - 1).astype(jnp.int32) for source in source_ids]

    def one_rank(packed):
        own_values, ghost_values, slot_map, cell_scale, masters, weights = packed
        return local_apply(own_values, ghost_values, slot_map, cell_scale, masters, weights, stiffness)

    def operate(vector):
        field_rows = vector.reshape(rank_count, NOWN)
        ghost_parts = []
        for neighbour in range(block_count):
            fetched = field_rows[owner_ids[neighbour][:, None], list_rows[owner_ids[neighbour], neighbour]]
            ghost_parts.append(jnp.where(inside[neighbour][:, None], fetched, 0.0))
        ghosts = jnp.stack(ghost_parts, axis=1)
        spread = lax.map(one_rank, (field_rows, ghosts, slot_maps, scales, master_maps, weight_maps))
        result = (spread[:, :NOWN] + reactions * field_rows).reshape(-1)
        returned = spread[:, NOWN:].reshape(rank_count, block_count, GHOSTS)
        for neighbour in range(block_count):
            target = owner_ids[neighbour][:, None] * NOWN + list_rows[owner_ids[neighbour], neighbour]
            addend = jnp.where(inside[neighbour][:, None], returned[:, neighbour], 0.0)
            result = result.at[target.reshape(-1)].add(addend.reshape(-1))
        return result
    solution = jnp.zeros_like(right_side)
    residual = right_side
    direction = right_side
    norm_now = jnp.sum(residual * residual)
    for iteration in range(ITERS):
        applied = operate(direction)
        step_size = norm_now / jnp.sum(direction * applied)
        solution = solution + step_size * direction
        residual = residual - step_size * applied
        norm_next = jnp.sum(residual * residual)
        direction = residual + norm_next / norm_now * direction
        norm_now = norm_next
    return (solution, residual)
```

```python
import functools

import jax
import jax.numpy as jnp
import numpy as np
from jax import lax
from jax.experimental import pallas as pl
from jax.experimental.pallas import tpu as pltpu
from jax.sharding import PartitionSpec as P

ITERS = 3
LANES = 128
MESH = pl.DeviceIdType.MESH


def lagrange(node_list, points):
    node_count = len(node_list)
    values = np.ones((len(points), node_count))
    derivs = np.zeros((len(points), node_count))
    for basis_node in range(node_count):
        for other_node in range(node_count):
            if other_node != basis_node:
                values[:, basis_node] = (
                    values[:, basis_node]
                    * (points - node_list[other_node])
                    / (node_list[basis_node] - node_list[other_node])
                )
        for skipped in range(node_count):
            if skipped != basis_node:
                product_term = np.ones(len(points)) / (node_list[basis_node] - node_list[skipped])
                for other_node in range(node_count):
                    if other_node != basis_node and other_node != skipped:
                        product_term = (
                            product_term
                            * (points - node_list[other_node])
                            / (node_list[basis_node] - node_list[other_node])
                        )
                derivs[:, basis_node] = derivs[:, basis_node] + product_term
    return (values, derivs)


def tables():
    gll_offset = np.sqrt(3.0 / 7.0)
    lobatto = np.array([0.0, (1.0 - gll_offset) / 2.0, 0.5, (1.0 + gll_offset) / 2.0, 1.0])
    inner_point = np.sqrt(5.0 - 2.0 * np.sqrt(10.0 / 7.0)) / 3.0
    outer_point = np.sqrt(5.0 + 2.0 * np.sqrt(10.0 / 7.0)) / 3.0
    inner_weight = (322.0 + 13.0 * np.sqrt(70.0)) / 900.0
    outer_weight = (322.0 - 13.0 * np.sqrt(70.0)) / 900.0
    points = np.array([-outer_point, -inner_point, 0.0, inner_point, outer_point])
    gauss_weights = np.array(
        [outer_weight, inner_weight, 128.0 / 225.0, inner_weight, outer_weight]
    )
    points = (points + 1.0) / 2.0
    gauss_weights = gauss_weights / 2.0
    shapes, slopes = lagrange(lobatto, points)
    fine_points = np.concatenate([lobatto / 2.0, (1.0 + lobatto) / 2.0])
    interp, unused_slopes = lagrange(lobatto, fine_points)
    quad_weights = np.kron(gauss_weights, np.kron(gauss_weights, gauss_weights))
    grad_x = np.kron(slopes, np.kron(shapes, shapes))
    grad_y = np.kron(shapes, np.kron(slopes, shapes))
    grad_z = np.kron(shapes, np.kron(shapes, slopes))
    stiffness = np.zeros((125, 125))
    for gradient in (grad_x, grad_y, grad_z):
        stiffness = stiffness + gradient.T @ (quad_weights[:, None] * gradient)
    return (interp.astype(np.float32), stiffness.astype(np.float32))


def round_up(value, step):
    return -(-value // step) * step


def split(value):
    high = value.astype(jnp.bfloat16)
    low = (value - high.astype(jnp.float32)).astype(jnp.bfloat16)
    return high, low


def kernel(
    shape,
    interp,
    right_ref,
    reaction_ref,
    cells_ref,
    level_ref,
    masters_ref,
    rows_ref,
    lists_ref,
    stiff_ref,
    solution_ref,
    residual_ref,
    table,
    onehot,
    lane_of,
    row_of,
    weights,
    cell_buf,
    acc,
    out_src,
    out_dst,
    back_src,
    back_dst,
    part,
    first_buf,
    mid_part,
    second_buf,
    out_send,
    out_recv,
    back_send,
    back_recv,
    first_send,
    first_recv,
    second_send,
    second_recv,
):
    nx, ny = shape
    count = nx * ny
    me = lax.axis_index("gx") * ny + lax.axis_index("gy")

    def place(rank):
        return (lax.div(rank, ny), lax.rem(rank, ny))

    blocks, listed = lists_ref.shape
    half = blocks // 2
    offsets = [j + 1 for j in range(half)] + [-(j + 1) for j in range(half)]
    own_rows = right_ref.shape[0]
    block_rows = listed // LANES
    ghost_rows = blocks * block_rows
    local_rows = own_rows + ghost_rows
    con_rows = rows_ref.shape[0]
    all_rows = round_up(local_rows + con_rows, 16)
    nodes = masters_ref.shape[0]
    points = cells_ref.shape[0]
    cell_rows = round_up(points, 8)
    cell_groups = cell_rows // 8
    list_groups = ghost_rows // 8
    list_base = cell_groups
    con_base = cell_groups + list_groups
    near = 1
    while near * near < count:
        near *= 2
    far = count // near
    near_id, far_id = lax.rem(me, near), lax.div(me, near)

    def near_peer(step):
        return far_id * near + lax.rem(near_id + step, near)

    def far_peer(step):
        return lax.rem(far_id + step, far) * near + near_id

    def ring_peer(offset):
        return lax.rem(me + offset + count, count)

    barrier = pltpu.get_barrier_semaphore()
    peers = [ring_peer(offset) for offset in offsets]
    peers += [near_peer(step) for step in range(1, near)]
    peers += [far_peer(step) for step in range(1, far)]
    for peer in peers:
        pl.semaphore_signal(barrier, inc=1, device_id=place(peer), device_id_type=MESH)

    lane_of[...] = jnp.zeros_like(lane_of)
    row_of[...] = jnp.full_like(row_of, -1)

    def put(at, slots):
        size = slots.shape[0]
        lane_of[at : at + size, :] = lax.rem(slots, LANES)
        row_of[at : at + size, :] = lax.div(slots, LANES)

    put(0, cells_ref[...])
    for j in range(blocks):
        for q in range(block_rows):
            put(list_base * 8 + j * block_rows + q, lists_ref[j : j + 1, q * LANES : (q + 1) * LANES])
    weights[...] = jnp.zeros_like(weights)
    for h in range(con_rows):
        put((con_base + h) * 8, masters_ref[:, h * LANES : (h + 1) * LANES])
        chosen = rows_ref[h : h + 1, :]
        for k in range(nodes):
            weight = jnp.zeros((1, LANES), jnp.float32)
            for t in range(interp.shape[0]):
                weight = jnp.where(chosen == t, float(interp[t, k]), weight)
            weights[h * 8 + k : h * 8 + k + 1, :] = weight

    lane_iota = lax.broadcasted_iota(jnp.int32, (LANES, LANES), 0)

    def build(g, carry):
        lanes = lane_of[pl.ds(pl.multiple_of(g * 8, 8), 8), :]
        for i in range(8):
            hit = jnp.where(lanes[i : i + 1, :] == lane_iota, 1.0, 0.0)
            onehot[g, :, i * LANES : (i + 1) * LANES] = hit.astype(jnp.bfloat16)
        return carry

    lax.fori_loop(0, onehot.shape[0], build, 0)
    table[...] = jnp.zeros_like(table)
    cell_buf[...] = jnp.zeros_like(cell_buf)
    scale = jnp.exp2(-level_ref[...].astype(jnp.float32))

    iota8 = lax.broadcasted_iota(jnp.int32, (8, LANES), 0)

    def gather(g, depth):
        hits = onehot[g]
        spread = jnp.dot(
            table[0:depth, :],
            jnp.concatenate([hits, hits], axis=0),
            preferred_element_type=jnp.float32,
        )
        rows = row_of[pl.ds(pl.multiple_of(g * 8, 8), 8), :]
        found = []
        for i in range(8):
            wanted = jnp.broadcast_to(rows[i : i + 1, :], (8, LANES)) - iota8
            picked = jnp.zeros((8, LANES), jnp.float32)
            for k in range(depth // 8):
                block = spread[8 * k : 8 * k + 8, i * LANES : (i + 1) * LANES]
                picked = jnp.where(wanted == 8 * k, block, picked)
            found.append(jnp.sum(picked, axis=0, keepdims=True))
        return jnp.concatenate(found, axis=0)

    def scatter(g, values, depth):
        rows = row_of[pl.ds(pl.multiple_of(g * 8, 8), 8), :]
        high = values.astype(jnp.bfloat16).astype(jnp.float32)
        low = values - high
        row_iota = lax.broadcasted_iota(jnp.int32, (depth, LANES), 0)
        columns = []
        for i in range(8):
            hit = rows[i : i + 1, :] == row_iota
            upper = jnp.where(hit, high[i : i + 1, :], 0.0).astype(jnp.bfloat16)
            lower = jnp.where(hit, low[i : i + 1, :], 0.0).astype(jnp.bfloat16)
            columns.append(jnp.concatenate([upper, lower], axis=0))
        placed = jnp.concatenate(columns, axis=1)
        return lax.dot_general(
            placed, onehot[g], (((1,), (1,)), ((), ())), preferred_element_type=jnp.float32
        )

    def store(at, value):
        high, low = split(value)
        size = value.shape[0]
        table[at : at + size, 0:LANES] = high
        table[at : at + size, LANES : 2 * LANES] = low

    def out_copy(turn, j):
        return pltpu.make_async_remote_copy(
            src_ref=out_src.at[turn, j],
            dst_ref=out_dst.at[turn, j],
            send_sem=out_send.at[turn, j],
            recv_sem=out_recv.at[turn, j],
            device_id=place(ring_peer(offsets[j])),
            device_id_type=MESH,
        )

    def back_copy(turn, j):
        return pltpu.make_async_remote_copy(
            src_ref=back_src.at[turn, j],
            dst_ref=back_dst.at[turn, j],
            send_sem=back_send.at[turn, j],
            recv_sem=back_recv.at[turn, j],
            device_id=place(ring_peer(-offsets[j])),
            device_id_type=MESH,
        )

    def near_copy(turn, step):
        return pltpu.make_async_remote_copy(
            src_ref=part.at[turn],
            dst_ref=first_buf.at[turn, near_id],
            send_sem=first_send.at[turn, step],
            recv_sem=first_recv.at[turn, step],
            device_id=place(near_peer(step)),
            device_id_type=MESH,
        )

    def far_copy(turn, step):
        return pltpu.make_async_remote_copy(
            src_ref=mid_part.at[turn],
            dst_ref=second_buf.at[turn, far_id],
            send_sem=second_send.at[turn, step],
            recv_sem=second_recv.at[turn, step],
            device_id=place(far_peer(step)),
            device_id_type=MESH,
        )

    def received(ref, turn, signs):
        rows = []
        for j in range(blocks):
            other = me + signs * offsets[j]
            inside = jnp.logical_and(other >= 0, other < count)
            rows.append(jnp.where(inside, ref[turn, j], 0.0))
        return jnp.concatenate(rows, axis=0)

    def apply(turn, vector, middle):
        store(0, vector)
        per_group = 8 // block_rows
        for q in range(list_groups):
            found = gather(list_base + q, own_rows)
            for r in range(per_group):
                j = q * per_group + r
                out_src[turn, j] = found[r * block_rows : (r + 1) * block_rows]
        for j in range(blocks):
            out_copy(turn, j).start()
        for j in range(blocks):
            out_copy(turn, j).wait()
        middle()
        store(own_rows, received(out_dst, turn, -1))
        resolved = []
        for h in range(con_rows):
            found = gather(con_base + h, local_rows)
            resolved.append(jnp.sum(weights[8 * h : 8 * h + 8, :] * found, axis=0, keepdims=True))
        spare = all_rows - local_rows - con_rows
        resolved.append(jnp.zeros((spare, LANES), jnp.float32))
        store(local_rows, jnp.concatenate(resolved, axis=0))

        def take(g, carry):
            cell_buf[pl.ds(pl.multiple_of(g * 8, 8), 8), :] = gather(g, all_rows)
            return carry

        lax.fori_loop(0, cell_groups, take, 0)
        contrib = jnp.dot(
            stiff_ref[...],
            cell_buf[...],
            precision=lax.Precision.HIGHEST,
            preferred_element_type=jnp.float32,
        )
        cell_buf[...] = contrib * scale
        acc[...] = jnp.zeros_like(acc)

        def give(g, carry):
            values = cell_buf[pl.ds(pl.multiple_of(g * 8, 8), 8), :]
            acc[...] += scatter(g, values, all_rows)
            return carry

        lax.fori_loop(0, cell_groups, give, 0)
        summed = acc[0:all_rows, :] + acc[all_rows : 2 * all_rows, :]
        spread = summed[0:local_rows]
        for h in range(con_rows):
            at = local_rows + h
            values = weights[8 * h : 8 * h + 8, :] * summed[at : at + 1]
            both = scatter(con_base + h, values, local_rows)
            spread = spread + both[0:local_rows] + both[local_rows : 2 * local_rows]
        for j in range(blocks):
            at = own_rows + j * block_rows
            back_src[turn, j] = spread[at : at + block_rows]
        for j in range(blocks):
            back_copy(turn, j).start()
        result = spread[0:own_rows] + reaction_ref[...] * vector
        for j in range(blocks):
            back_copy(turn, j).wait()
        values = received(back_dst, turn, 1)
        for q in range(list_groups):
            both = scatter(list_base + q, values[8 * q : 8 * q + 8], own_rows)
            result = result + both[0:own_rows] + both[own_rows : 2 * own_rows]
        return result

    def sums_start(turn, vector, applied):
        mine = jnp.concatenate(
            [
                jnp.sum(vector * vector, axis=0, keepdims=True),
                jnp.sum(vector * applied, axis=0, keepdims=True),
            ],
            axis=0,
        )
        part[turn] = mine
        first_buf[turn, near_id] = mine
        for step in range(1, near):
            near_copy(turn, step).start()

    def sums_middle(turn):
        for step in range(1, near):
            near_copy(turn, step).wait()
        mine = first_buf[turn, 0]
        for k in range(1, near):
            mine = mine + first_buf[turn, k]
        mid_part[turn] = mine
        second_buf[turn, far_id] = mine
        for step in range(1, far):
            far_copy(turn, step).start()

    def sums_end(turn):
        for step in range(1, far):
            far_copy(turn, step).wait()
        total = second_buf[turn, 0]
        for k in range(1, far):
            total = total + second_buf[turn, k]
        total = jnp.sum(total, axis=1, keepdims=True)
        return total[0:1], total[1:2]

    pl.semaphore_wait(barrier, len(peers))

    residual = right_ref[...]
    applied = apply(0, residual, lambda: None)
    answer = direction = applied_dir = twice_dir = None
    norm_before = step_before = None
    for turn in range(ITERS):
        sums_start(turn, residual, applied)
        last = turn + 1 == ITERS
        if last:
            sums_middle(turn)
        else:
            twice = apply(turn + 1, applied, functools.partial(sums_middle, turn))
        norm, product = sums_end(turn)
        if turn == 0:
            step_size = norm / product
            direction, applied_dir = residual, applied
            if not last:
                twice_dir = twice
            answer = step_size * direction
        else:
            ratio = norm / norm_before
            step_size = norm / (product - ratio * norm / step_before)
            direction = residual + ratio * direction
            applied_dir = applied + ratio * applied_dir
            if not last:
                twice_dir = twice + ratio * twice_dir
            answer = answer + step_size * direction
        residual = residual - step_size * applied_dir
        if not last:
            applied = applied - step_size * twice_dir
        norm_before, step_before = norm, step_size
    solution_ref[...] = answer
    residual_ref[...] = residual


def on_device(shape, right_side, reaction, cell_slots, cell_level, con_masters, con_rows, send_lists):
    interp, stiffness = tables()
    own = right_side.shape[0]
    own_rows = own // LANES
    blocks, listed = send_lists.shape
    block_rows = listed // LANES
    con_tiles = con_rows.shape[0] // LANES
    points = cell_slots.shape[0]
    cell_rows = round_up(points, 8)
    all_rows = round_up(own_rows + blocks * block_rows + con_tiles, 16)
    groups = cell_rows // 8 + blocks * block_rows // 8 + con_tiles
    padded = np.zeros((cell_rows, cell_rows), np.float32)
    padded[:points, :points] = stiffness
    count = shape[0] * shape[1]
    near = 1
    while near * near < count:
        near *= 2
    far = count // near
    exchange = pltpu.VMEM((ITERS, blocks, block_rows, LANES), jnp.float32)
    tile = jax.ShapeDtypeStruct((own_rows, LANES), jnp.float32)
    answer, residual = pl.pallas_call(
        functools.partial(kernel, shape, interp),
        out_shape=(tile, tile),
        in_specs=[pl.BlockSpec(memory_space=pltpu.VMEM)] * 8,
        out_specs=(pl.BlockSpec(memory_space=pltpu.VMEM),) * 2,
        scratch_shapes=[
            pltpu.VMEM((all_rows, 2 * LANES), jnp.bfloat16),
            pltpu.VMEM((groups, LANES, 8 * LANES), jnp.bfloat16),
            pltpu.VMEM((groups * 8, LANES), jnp.int32),
            pltpu.VMEM((groups * 8, LANES), jnp.int32),
            pltpu.VMEM((con_tiles * 8, LANES), jnp.float32),
            pltpu.VMEM((cell_rows, LANES), jnp.float32),
            pltpu.VMEM((2 * all_rows, LANES), jnp.float32),
            exchange,
            exchange,
            exchange,
            exchange,
            pltpu.VMEM((ITERS, 2, LANES), jnp.float32),
            pltpu.VMEM((ITERS, near, 2, LANES), jnp.float32),
            pltpu.VMEM((ITERS, 2, LANES), jnp.float32),
            pltpu.VMEM((ITERS, far, 2, LANES), jnp.float32),
            pltpu.SemaphoreType.DMA((ITERS, blocks)),
            pltpu.SemaphoreType.DMA((ITERS, blocks)),
            pltpu.SemaphoreType.DMA((ITERS, blocks)),
            pltpu.SemaphoreType.DMA((ITERS, blocks)),
            pltpu.SemaphoreType.DMA((ITERS, near)),
            pltpu.SemaphoreType.DMA((ITERS, near)),
            pltpu.SemaphoreType.DMA((ITERS, far)),
            pltpu.SemaphoreType.DMA((ITERS, far)),
        ],
        compiler_params=pltpu.CompilerParams(
            collective_id=0, has_side_effects=True, vmem_limit_bytes=40 * 1024 * 1024
        ),
    )(
        right_side.reshape(own_rows, LANES),
        reaction.reshape(own_rows, LANES),
        cell_slots,
        cell_level.reshape(1, -1),
        con_masters,
        con_rows.reshape(con_tiles, LANES),
        send_lists,
        jnp.asarray(padded),
    )
    return (answer.reshape(own), residual.reshape(own))


def solution(mesh):
    placed = (
        P(("gx", "gy")),
        P(("gx", "gy")),
        P(None, ("gx", "gy")),
        P(("gx", "gy")),
        P(None, ("gx", "gy")),
        P(("gx", "gy")),
        P(None, ("gx", "gy")),
    )
    return jax.shard_map(
        functools.partial(on_device, (mesh.shape["gx"], mesh.shape["gy"])),
        mesh=mesh,
        in_specs=placed,
        out_specs=(P(("gx", "gy")), P(("gx", "gy"))),
        check_vma=False,
    )
```

```python
import functools

import jax
import jax.numpy as jnp
import numpy as np
from jax import lax
from jax.experimental import pallas as pl
from jax.experimental.pallas import tpu as pltpu
from jax.sharding import PartitionSpec as P

ITERS = 3
LANES = 128
SUMS = 4
ROUNDS = 2
MESH = pl.DeviceIdType.MESH


def lagrange(node_list, points):
    node_count = len(node_list)
    values = np.ones((len(points), node_count))
    derivs = np.zeros((len(points), node_count))
    for basis_node in range(node_count):
        for other_node in range(node_count):
            if other_node != basis_node:
                values[:, basis_node] = (
                    values[:, basis_node]
                    * (points - node_list[other_node])
                    / (node_list[basis_node] - node_list[other_node])
                )
        for skipped in range(node_count):
            if skipped != basis_node:
                product_term = np.ones(len(points)) / (node_list[basis_node] - node_list[skipped])
                for other_node in range(node_count):
                    if other_node != basis_node and other_node != skipped:
                        product_term = (
                            product_term
                            * (points - node_list[other_node])
                            / (node_list[basis_node] - node_list[other_node])
                        )
                derivs[:, basis_node] = derivs[:, basis_node] + product_term
    return (values, derivs)


def tables():
    gll_offset = np.sqrt(3.0 / 7.0)
    lobatto = np.array([0.0, (1.0 - gll_offset) / 2.0, 0.5, (1.0 + gll_offset) / 2.0, 1.0])
    inner_point = np.sqrt(5.0 - 2.0 * np.sqrt(10.0 / 7.0)) / 3.0
    outer_point = np.sqrt(5.0 + 2.0 * np.sqrt(10.0 / 7.0)) / 3.0
    inner_weight = (322.0 + 13.0 * np.sqrt(70.0)) / 900.0
    outer_weight = (322.0 - 13.0 * np.sqrt(70.0)) / 900.0
    points = np.array([-outer_point, -inner_point, 0.0, inner_point, outer_point])
    gauss_weights = np.array(
        [outer_weight, inner_weight, 128.0 / 225.0, inner_weight, outer_weight]
    )
    points = (points + 1.0) / 2.0
    gauss_weights = gauss_weights / 2.0
    shapes, slopes = lagrange(lobatto, points)
    fine_points = np.concatenate([lobatto / 2.0, (1.0 + lobatto) / 2.0])
    interp, unused_slopes = lagrange(lobatto, fine_points)
    quad_weights = np.kron(gauss_weights, np.kron(gauss_weights, gauss_weights))
    grad_x = np.kron(slopes, np.kron(shapes, shapes))
    grad_y = np.kron(shapes, np.kron(slopes, shapes))
    grad_z = np.kron(shapes, np.kron(shapes, slopes))
    stiffness = np.zeros((125, 125))
    for gradient in (grad_x, grad_y, grad_z):
        stiffness = stiffness + gradient.T @ (quad_weights[:, None] * gradient)
    return (interp.astype(np.float32), stiffness.astype(np.float32))


def round_up(value, step):
    return -(-value // step) * step


def split(value):
    high = value.astype(jnp.bfloat16)
    low = (value - high.astype(jnp.float32)).astype(jnp.bfloat16)
    return high, low


def kernel(
    shape,
    interp,
    *refs,
):
    inputs, refs = refs[:8], refs[8:]
    solution_ref, residual_ref = refs[:2]
    staged, refs = refs[2:10], refs[10:]
    right_ref, reaction_ref, cells_ref, level_ref, masters_ref, rows_ref, lists_ref, stiff_ref = staged
    (
    load_sem,
    own_table,
    ghost_table,
    onehot,
    lane_of,
    row_of,
    weights,
    cell_buf,
    own_acc,
    ghost_acc,
    out_src,
    out_dst,
    back_src,
    back_dst,
    part,
    first_buf,
    mid_part,
    second_buf,
    out_send,
    out_recv,
    back_send,
    back_recv,
    first_send,
    first_recv,
    second_send,
    second_recv,
    ) = refs
    loads = [
        pltpu.make_async_copy(source, target, load_sem.at[i])
        for i, (source, target) in enumerate(zip(inputs, staged))
    ]
    for load in loads:
        load.start()
    nx, ny = shape
    count = nx * ny
    me = lax.axis_index("gx") * ny + lax.axis_index("gy")

    def place(rank):
        return (lax.div(rank, ny), lax.rem(rank, ny))

    blocks, listed = lists_ref.shape
    half = blocks // 2
    offsets = [j + 1 for j in range(half)] + [-(j + 1) for j in range(half)]
    own_rows = right_ref.shape[0]
    block_rows = listed // LANES
    ghost_rows = blocks * block_rows
    local_rows = own_rows + ghost_rows
    con_rows = rows_ref.shape[0]
    far_rows = round_up(ghost_rows + con_rows, 16)
    nodes = masters_ref.shape[0]
    points = cells_ref.shape[0]
    cell_rows = round_up(points, 8)
    cell_groups = cell_rows // 8
    list_groups = ghost_rows // 8
    list_base = cell_groups
    con_base = cell_groups + list_groups
    near = 1
    while near * near < count:
        near *= 2
    far = count // near
    near_id, far_id = lax.rem(me, near), lax.div(me, near)

    def near_peer(step):
        return far_id * near + lax.rem(near_id + step, near)

    def far_peer(step):
        return lax.rem(far_id + step, far) * near + near_id

    def ring_peer(offset):
        return lax.rem(me + offset + count, count)

    barrier = pltpu.get_barrier_semaphore()
    peers = [ring_peer(offset) for offset in offsets]
    peers += [near_peer(step) for step in range(1, near)]
    peers += [far_peer(step) for step in range(1, far)]
    for peer in peers:
        pl.semaphore_signal(barrier, inc=1, device_id=place(peer), device_id_type=MESH)

    for load in loads:
        load.wait()
    lane_of[...] = jnp.zeros_like(lane_of)
    row_of[...] = jnp.full_like(row_of, -1)

    def put(at, slots):
        size = slots.shape[0]
        lane_of[at : at + size, :] = lax.rem(slots, LANES)
        row_of[at : at + size, :] = lax.div(slots, LANES)

    put(0, cells_ref[...])
    for j in range(blocks):
        for q in range(block_rows):
            put(list_base * 8 + j * block_rows + q, lists_ref[j : j + 1, q * LANES : (q + 1) * LANES])
    weights[...] = jnp.zeros_like(weights)
    for h in range(con_rows):
        put((con_base + h) * 8, masters_ref[:, h * LANES : (h + 1) * LANES])
        chosen = rows_ref[h : h + 1, :]
        for k in range(nodes):
            weight = jnp.zeros((1, LANES), jnp.float32)
            for t in range(interp.shape[0]):
                weight = jnp.where(chosen == t, float(interp[t, k]), weight)
            weights[h * 8 + k : h * 8 + k + 1, :] = weight

    lane_iota = lax.broadcasted_iota(jnp.int32, (LANES, LANES), 0)

    def build(g, carry):
        lanes = lane_of[pl.ds(pl.multiple_of(g * 8, 8), 8), :]
        for i in range(8):
            hit = jnp.where(lanes[i : i + 1, :] == lane_iota, 1.0, 0.0)
            onehot[g, :, i * LANES : (i + 1) * LANES] = hit.astype(jnp.bfloat16)
        return carry

    lax.fori_loop(0, onehot.shape[0], build, 0)
    cell_buf[...] = jnp.zeros_like(cell_buf)
    scale = jnp.exp2(-level_ref[...].astype(jnp.float32))

    iota8 = lax.broadcasted_iota(jnp.int32, (8, LANES), 0)

    def gather(g, table, base, depth):
        stacked = table.shape[0] // 2
        pieces = [table[0:depth, :], table[stacked : stacked + depth, :]]
        left = table[...] if depth == stacked else jnp.concatenate(pieces, axis=0)
        spread = jnp.dot(left, onehot[g], preferred_element_type=jnp.float32)
        rows = row_of[pl.ds(pl.multiple_of(g * 8, 8), 8), :] - base
        found = []
        for i in range(8):
            wanted = jnp.broadcast_to(rows[i : i + 1, :], (8, LANES)) - iota8
            high = jnp.zeros((8, LANES), jnp.float32)
            low = high
            for k in range(depth // 8):
                hit = wanted == 8 * k
                at, cols = 8 * k, slice(i * LANES, (i + 1) * LANES)
                high = jnp.where(hit, spread[at : at + 8, cols], high)
                low = jnp.where(hit, spread[depth + at : depth + at + 8, cols], low)
            found.append(jnp.sum(high + low, axis=0, keepdims=True))
        return jnp.concatenate(found, axis=0)

    def scatter(g, values, base, depth):
        rows = row_of[pl.ds(pl.multiple_of(g * 8, 8), 8), :] - base
        high = values.astype(jnp.bfloat16).astype(jnp.float32)
        low = values - high
        row_iota = lax.broadcasted_iota(jnp.int32, (depth, LANES), 0)
        columns = []
        for i in range(8):
            hit = rows[i : i + 1, :] == row_iota
            upper = jnp.where(hit, high[i : i + 1, :], 0.0).astype(jnp.bfloat16)
            lower = jnp.where(hit, low[i : i + 1, :], 0.0).astype(jnp.bfloat16)
            columns.append(jnp.concatenate([upper, lower], axis=0))
        placed = jnp.concatenate(columns, axis=1)
        return lax.dot_general(
            placed, onehot[g], (((1,), (1,)), ((), ())), preferred_element_type=jnp.float32
        )

    def folded(both):
        depth = both.shape[0] // 2
        return both[0:depth] + both[depth : 2 * depth]

    def store(table, value):
        high, low = split(value)
        size = value.shape[0]
        table[0:size, :] = high
        table[size : 2 * size, :] = low

    def out_copy(turn, j):
        return pltpu.make_async_remote_copy(
            src_ref=out_src.at[turn, j],
            dst_ref=out_dst.at[turn, j],
            send_sem=out_send.at[turn, j],
            recv_sem=out_recv.at[turn, j],
            device_id=place(ring_peer(offsets[j])),
            device_id_type=MESH,
        )

    def back_copy(turn, j):
        return pltpu.make_async_remote_copy(
            src_ref=back_src.at[turn, j],
            dst_ref=back_dst.at[turn, j],
            send_sem=back_send.at[turn, j],
            recv_sem=back_recv.at[turn, j],
            device_id=place(ring_peer(-offsets[j])),
            device_id_type=MESH,
        )

    def near_copy(turn, step):
        return pltpu.make_async_remote_copy(
            src_ref=part.at[turn],
            dst_ref=first_buf.at[turn, near_id],
            send_sem=first_send.at[turn, step],
            recv_sem=first_recv.at[turn, step],
            device_id=place(near_peer(step)),
            device_id_type=MESH,
        )

    def far_copy(turn, step):
        return pltpu.make_async_remote_copy(
            src_ref=mid_part.at[turn],
            dst_ref=second_buf.at[turn, far_id],
            send_sem=second_send.at[turn, step],
            recv_sem=second_recv.at[turn, step],
            device_id=place(far_peer(step)),
            device_id_type=MESH,
        )

    def received(ref, turn, signs):
        rows = []
        for j in range(blocks):
            other = me + signs * offsets[j]
            inside = jnp.logical_and(other >= 0, other < count)
            rows.append(jnp.where(inside, ref[turn, j], 0.0))
        return jnp.concatenate(rows, axis=0)

    def group(g):
        return pl.ds(pl.multiple_of(g * 8, 8), 8)

    def apply(turn, vector, begin, middle):
        store(own_table, vector)
        per_group = 8 // block_rows
        for q in range(list_groups):
            found = gather(list_base + q, own_table, 0, own_rows)
            for r in range(per_group):
                j = q * per_group + r
                out_src[turn, j] = found[r * block_rows : (r + 1) * block_rows]
        if turn == 0:
            pl.semaphore_wait(barrier, len(peers))
        for j in range(blocks):
            out_copy(turn, j).start()

        def take_own(g, carry):
            cell_buf[group(g), :] = gather(g, own_table, 0, own_rows)
            return carry

        lax.fori_loop(0, cell_groups, take_own, 0)
        con_own = [gather(con_base + h, own_table, 0, own_rows) for h in range(con_rows)]
        for j in range(blocks):
            out_copy(turn, j).wait()
        ghosts = received(out_dst, turn, -1)
        padding = jnp.zeros((far_rows - ghost_rows, LANES), jnp.float32)
        store(ghost_table, jnp.concatenate([ghosts, padding], axis=0))
        resolved = []
        for h in range(con_rows):
            found = con_own[h] + gather(con_base + h, ghost_table, own_rows, ghost_rows)
            resolved.append(jnp.sum(weights[8 * h : 8 * h + 8, :] * found, axis=0, keepdims=True))
        resolved.append(jnp.zeros((far_rows - ghost_rows - con_rows, LANES), jnp.float32))
        store(ghost_table, jnp.concatenate([ghosts] + resolved, axis=0))

        def take_far(g, carry):
            cell_buf[group(g), :] += gather(g, ghost_table, own_rows, far_rows)
            return carry

        lax.fori_loop(0, cell_groups, take_far, 0)
        nodal = cell_buf[...]
        contrib = scale * jnp.dot(
            stiff_ref[...],
            nodal,
            precision=lax.Precision.HIGHEST,
            preferred_element_type=jnp.float32,
        )
        cell_buf[...] = contrib
        weighted = reaction_ref[...] * vector
        energy = jnp.sum(nodal * contrib, axis=0, keepdims=True)
        energy = energy + jnp.sum(weighted * vector, axis=0, keepdims=True)
        begin(energy)
        ghost_acc[...] = jnp.zeros_like(ghost_acc)

        def give_far(g, carry):
            ghost_acc[...] += scatter(g, cell_buf[group(g), :], own_rows, far_rows)
            return carry

        lax.fori_loop(0, cell_groups, give_far, 0)
        summed = folded(ghost_acc[...])
        spread = summed[0:ghost_rows]
        shares = []
        for h in range(con_rows):
            at = ghost_rows + h
            shares.append(weights[8 * h : 8 * h + 8, :] * summed[at : at + 1])
            spread = spread + folded(scatter(con_base + h, shares[h], own_rows, ghost_rows))
        for j in range(blocks):
            back_src[turn, j] = spread[j * block_rows : (j + 1) * block_rows]
        for j in range(blocks):
            back_copy(turn, j).start()
        middle()
        own_acc[...] = jnp.zeros_like(own_acc)

        def give_own(g, carry):
            own_acc[...] += scatter(g, cell_buf[group(g), :], 0, own_rows)
            return carry

        lax.fori_loop(0, cell_groups, give_own, 0)
        both = own_acc[...]
        for h in range(con_rows):
            both = both + scatter(con_base + h, shares[h], 0, own_rows)
        for j in range(blocks):
            back_copy(turn, j).wait()
        values = received(back_dst, turn, 1)
        for q in range(list_groups):
            both = both + scatter(list_base + q, values[8 * q : 8 * q + 8], 0, own_rows)
        return folded(both) + weighted

    def dot(one, two):
        return jnp.sum(one * two, axis=0, keepdims=True)

    def sums_start(turn, parts):
        mine = jnp.concatenate(parts, axis=0)
        part[turn] = mine
        first_buf[turn, near_id] = mine
        for step in range(1, near):
            near_copy(turn, step).start()

    def sums_middle(turn):
        for step in range(1, near):
            near_copy(turn, step).wait()
        mine = first_buf[turn, 0]
        for k in range(1, near):
            mine = mine + first_buf[turn, k]
        mid_part[turn] = mine
        second_buf[turn, far_id] = mine
        for step in range(1, far):
            far_copy(turn, step).start()

    def sums_end(turn):
        for step in range(1, far):
            far_copy(turn, step).wait()
        total = second_buf[turn, 0]
        for k in range(1, far):
            total = total + second_buf[turn, k]
        total = jnp.sum(total, axis=1, keepdims=True)
        return [total[k : k + 1] for k in range(SUMS)]

    start = right_ref[...]
    first = apply(0, start, lambda energy: None, lambda: None)
    known = [dot(start, start), dot(start, first), dot(first, first)]
    second = apply(
        1,
        first,
        lambda energy: sums_start(0, known + [energy]),
        lambda: sums_middle(0),
    )
    m0, m1, m2, m3 = sums_end(0)
    step0 = m0 / m1
    norm1 = m0 - 2.0 * step0 * m1 + step0 * step0 * m2
    product1 = m1 - 2.0 * step0 * m2 + step0 * step0 * m3
    ratio1 = norm1 / m0
    step1 = norm1 / (product1 - ratio1 * norm1 / step0)
    residual = start - step0 * first
    applied = first - step0 * second
    direction = residual + ratio1 * start
    applied_dir = applied + ratio1 * first
    answer = step0 * start + step1 * direction
    residual = residual - step1 * applied_dir
    zero = jnp.zeros((1, LANES), jnp.float32)
    square = dot(residual, residual)
    applied = apply(
        2,
        residual,
        lambda energy: sums_start(1, [square, energy, zero, zero]),
        lambda: sums_middle(1),
    )
    norm2, product2, unused_a, unused_b = sums_end(1)
    ratio2 = norm2 / norm1
    step2 = norm2 / (product2 - ratio2 * norm2 / step1)
    solution_ref[...] = answer + step2 * (residual + ratio2 * direction)
    residual_ref[...] = residual - step2 * (applied + ratio2 * applied_dir)


def on_device(shape, right_side, reaction, cell_slots, cell_level, con_masters, con_rows, send_lists):
    interp, stiffness = tables()
    own = right_side.shape[0]
    own_rows = own // LANES
    blocks, listed = send_lists.shape
    block_rows = listed // LANES
    con_tiles = con_rows.shape[0] // LANES
    points = cell_slots.shape[0]
    cell_rows = round_up(points, 8)
    far_rows = round_up(blocks * block_rows + con_tiles, 16)
    groups = cell_rows // 8 + blocks * block_rows // 8 + con_tiles
    padded = np.zeros((cell_rows, cell_rows), np.float32)
    padded[:points, :points] = stiffness
    count = shape[0] * shape[1]
    near = 1
    while near * near < count:
        near *= 2
    far = count // near
    operands = [
        right_side.reshape(own_rows, LANES),
        reaction.reshape(own_rows, LANES),
        cell_slots,
        cell_level.reshape(1, -1),
        con_masters,
        con_rows.reshape(con_tiles, LANES),
        send_lists,
        jnp.asarray(padded),
    ]
    exchange = pltpu.VMEM((ITERS, blocks, block_rows, LANES), jnp.float32)
    tile = jax.ShapeDtypeStruct((own_rows, LANES), jnp.float32)
    answer, residual = pl.pallas_call(
        functools.partial(kernel, shape, interp),
        out_shape=(tile, tile),
        in_specs=[pl.BlockSpec(memory_space=pl.ANY)] * 8,
        out_specs=(pl.BlockSpec(memory_space=pltpu.VMEM),) * 2,
        scratch_shapes=[
            *[pltpu.VMEM(value.shape, value.dtype) for value in operands],
            pltpu.SemaphoreType.DMA((len(operands),)),
            pltpu.VMEM((2 * own_rows, LANES), jnp.bfloat16),
            pltpu.VMEM((2 * far_rows, LANES), jnp.bfloat16),
            pltpu.VMEM((groups, LANES, 8 * LANES), jnp.bfloat16),
            pltpu.VMEM((groups * 8, LANES), jnp.int32),
            pltpu.VMEM((groups * 8, LANES), jnp.int32),
            pltpu.VMEM((con_tiles * 8, LANES), jnp.float32),
            pltpu.VMEM((cell_rows, LANES), jnp.float32),
            pltpu.VMEM((2 * own_rows, LANES), jnp.float32),
            pltpu.VMEM((2 * far_rows, LANES), jnp.float32),
            exchange,
            exchange,
            exchange,
            exchange,
            pltpu.VMEM((ROUNDS, SUMS, LANES), jnp.float32),
            pltpu.VMEM((ROUNDS, near, SUMS, LANES), jnp.float32),
            pltpu.VMEM((ROUNDS, SUMS, LANES), jnp.float32),
            pltpu.VMEM((ROUNDS, far, SUMS, LANES), jnp.float32),
            pltpu.SemaphoreType.DMA((ITERS, blocks)),
            pltpu.SemaphoreType.DMA((ITERS, blocks)),
            pltpu.SemaphoreType.DMA((ITERS, blocks)),
            pltpu.SemaphoreType.DMA((ITERS, blocks)),
            pltpu.SemaphoreType.DMA((ROUNDS, near)),
            pltpu.SemaphoreType.DMA((ROUNDS, near)),
            pltpu.SemaphoreType.DMA((ROUNDS, far)),
            pltpu.SemaphoreType.DMA((ROUNDS, far)),
        ],
        compiler_params=pltpu.CompilerParams(
            collective_id=0, has_side_effects=True, vmem_limit_bytes=60 * 1024 * 1024
        ),
    )(*operands)
    return (answer.reshape(own), residual.reshape(own))


def solution(mesh):
    placed = (
        P(("gx", "gy")),
        P(("gx", "gy")),
        P(None, ("gx", "gy")),
        P(("gx", "gy")),
        P(None, ("gx", "gy")),
        P(("gx", "gy")),
        P(None, ("gx", "gy")),
    )
    return jax.shard_map(
        functools.partial(on_device, (mesh.shape["gx"], mesh.shape["gy"])),
        mesh=mesh,
        in_specs=placed,
        out_specs=(P(("gx", "gy")), P(("gx", "gy"))),
        check_vma=False,
    )
```

```python
import functools

import jax
import jax.numpy as jnp
import numpy as np
from jax import lax
from jax.experimental import pallas as pl
from jax.experimental.pallas import tpu as pltpu
from jax.sharding import PartitionSpec as P

ITERS = 3
LANES = 128
SUMS = 4
ROUNDS = 2
UNROLL = 8
MESH = pl.DeviceIdType.MESH


def lagrange(node_list, points):
    node_count = len(node_list)
    values = np.ones((len(points), node_count))
    derivs = np.zeros((len(points), node_count))
    for basis_node in range(node_count):
        for other_node in range(node_count):
            if other_node != basis_node:
                values[:, basis_node] = (
                    values[:, basis_node]
                    * (points - node_list[other_node])
                    / (node_list[basis_node] - node_list[other_node])
                )
        for skipped in range(node_count):
            if skipped != basis_node:
                product_term = np.ones(len(points)) / (node_list[basis_node] - node_list[skipped])
                for other_node in range(node_count):
                    if other_node != basis_node and other_node != skipped:
                        product_term = (
                            product_term
                            * (points - node_list[other_node])
                            / (node_list[basis_node] - node_list[other_node])
                        )
                derivs[:, basis_node] = derivs[:, basis_node] + product_term
    return (values, derivs)


def tables():
    gll_offset = np.sqrt(3.0 / 7.0)
    lobatto = np.array([0.0, (1.0 - gll_offset) / 2.0, 0.5, (1.0 + gll_offset) / 2.0, 1.0])
    inner_point = np.sqrt(5.0 - 2.0 * np.sqrt(10.0 / 7.0)) / 3.0
    outer_point = np.sqrt(5.0 + 2.0 * np.sqrt(10.0 / 7.0)) / 3.0
    inner_weight = (322.0 + 13.0 * np.sqrt(70.0)) / 900.0
    outer_weight = (322.0 - 13.0 * np.sqrt(70.0)) / 900.0
    points = np.array([-outer_point, -inner_point, 0.0, inner_point, outer_point])
    gauss_weights = np.array(
        [outer_weight, inner_weight, 128.0 / 225.0, inner_weight, outer_weight]
    )
    points = (points + 1.0) / 2.0
    gauss_weights = gauss_weights / 2.0
    shapes, slopes = lagrange(lobatto, points)
    fine_points = np.concatenate([lobatto / 2.0, (1.0 + lobatto) / 2.0])
    interp, unused_slopes = lagrange(lobatto, fine_points)
    quad_weights = np.kron(gauss_weights, np.kron(gauss_weights, gauss_weights))
    grad_x = np.kron(slopes, np.kron(shapes, shapes))
    grad_y = np.kron(shapes, np.kron(slopes, shapes))
    grad_z = np.kron(shapes, np.kron(shapes, slopes))
    stiffness = np.zeros((125, 125))
    for gradient in (grad_x, grad_y, grad_z):
        stiffness = stiffness + gradient.T @ (quad_weights[:, None] * gradient)
    return (interp.astype(np.float32), stiffness.astype(np.float32))


def round_up(value, step):
    return -(-value // step) * step


def split(value):
    high = value.astype(jnp.bfloat16)
    low = (value - high.astype(jnp.float32)).astype(jnp.bfloat16)
    return high, low


def kernel(
    shape,
    interp,
    *refs,
):
    inputs, refs = refs[:8], refs[8:]
    solution_ref, residual_ref = refs[:2]
    staged, refs = refs[2:10], refs[10:]
    right_ref, reaction_ref, cells_ref, level_ref, masters_ref, rows_ref, lists_ref, stiff_ref = staged
    (
    load_sem,
    own_table,
    ghost_table,
    onehot,
    lane_of,
    row_of,
    weights,
    cell_buf,
    own_acc,
    ghost_acc,
    out_src,
    out_dst,
    back_src,
    back_dst,
    part,
    first_buf,
    mid_part,
    second_buf,
    out_send,
    out_recv,
    back_send,
    back_recv,
    first_send,
    first_recv,
    second_send,
    second_recv,
    ) = refs
    loads = [
        pltpu.make_async_copy(source, target, load_sem.at[i])
        for i, (source, target) in enumerate(zip(inputs, staged))
    ]
    for load in loads:
        load.start()
    nx, ny = shape
    count = nx * ny
    me = lax.axis_index("gx") * ny + lax.axis_index("gy")

    def place(rank):
        return (lax.div(rank, ny), lax.rem(rank, ny))

    blocks, listed = lists_ref.shape
    half = blocks // 2
    offsets = [j + 1 for j in range(half)] + [-(j + 1) for j in range(half)]
    own_rows = right_ref.shape[0]
    block_rows = listed // LANES
    ghost_rows = blocks * block_rows
    local_rows = own_rows + ghost_rows
    con_rows = rows_ref.shape[0]
    far_rows = round_up(ghost_rows + con_rows, 16)
    nodes = masters_ref.shape[0]
    points = cells_ref.shape[0]
    cell_rows = round_up(points, 8)
    cell_groups = cell_rows // 8
    list_groups = ghost_rows // 8
    list_base = cell_groups
    con_base = cell_groups + list_groups
    near = 1
    while near * near < count:
        near *= 2
    far = count // near
    near_id, far_id = lax.rem(me, near), lax.div(me, near)

    def near_peer(step):
        return far_id * near + lax.rem(near_id + step, near)

    def far_peer(step):
        return lax.rem(far_id + step, far) * near + near_id

    def ring_peer(offset):
        return lax.rem(me + offset + count, count)

    barrier = pltpu.get_barrier_semaphore()
    peers = [ring_peer(offset) for offset in offsets]
    peers += [near_peer(step) for step in range(1, near)]
    peers += [far_peer(step) for step in range(1, far)]
    for peer in peers:
        pl.semaphore_signal(barrier, inc=1, device_id=place(peer), device_id_type=MESH)

    for load in loads:
        load.wait()
    lane_of[...] = jnp.zeros_like(lane_of)
    row_of[...] = jnp.full_like(row_of, -1)

    def put(at, slots):
        size = slots.shape[0]
        lane_of[at : at + size, :] = lax.rem(slots, LANES)
        row_of[at : at + size, :] = lax.div(slots, LANES)

    put(0, cells_ref[...])
    for j in range(blocks):
        for q in range(block_rows):
            put(list_base * 8 + j * block_rows + q, lists_ref[j : j + 1, q * LANES : (q + 1) * LANES])
    weights[...] = jnp.zeros_like(weights)
    for h in range(con_rows):
        put((con_base + h) * 8, masters_ref[:, h * LANES : (h + 1) * LANES])
        chosen = rows_ref[h : h + 1, :]
        for k in range(nodes):
            weight = jnp.zeros((1, LANES), jnp.float32)
            for t in range(interp.shape[0]):
                weight = jnp.where(chosen == t, float(interp[t, k]), weight)
            weights[h * 8 + k : h * 8 + k + 1, :] = weight

    lane_iota = lax.broadcasted_iota(jnp.int32, (LANES, LANES), 0)

    def build(g, carry):
        lanes = lane_of[pl.ds(pl.multiple_of(g * 8, 8), 8), :]
        for i in range(8):
            hit = jnp.where(lanes[i : i + 1, :] == lane_iota, 1.0, 0.0)
            onehot[g, :, i * LANES : (i + 1) * LANES] = hit.astype(jnp.bfloat16)
        return carry

    lax.fori_loop(0, onehot.shape[0], build, 0)
    cell_buf[...] = jnp.zeros_like(cell_buf)
    scale = jnp.exp2(-level_ref[...].astype(jnp.float32))

    iota8 = lax.broadcasted_iota(jnp.int32, (8, LANES), 0)

    def gather(g, table, base, depth):
        stacked = table.shape[0] // 2
        pieces = [table[0:depth, :], table[stacked : stacked + depth, :]]
        left = table[...] if depth == stacked else jnp.concatenate(pieces, axis=0)
        spread = jnp.dot(left, onehot[g], preferred_element_type=jnp.float32)
        rows = row_of[pl.ds(pl.multiple_of(g * 8, 8), 8), :] - base
        found = []
        for i in range(8):
            wanted = jnp.broadcast_to(rows[i : i + 1, :], (8, LANES)) - iota8
            high = jnp.zeros((8, LANES), jnp.float32)
            low = high
            for k in range(depth // 8):
                hit = wanted == 8 * k
                at, cols = 8 * k, slice(i * LANES, (i + 1) * LANES)
                high = jnp.where(hit, spread[at : at + 8, cols], high)
                low = jnp.where(hit, spread[depth + at : depth + at + 8, cols], low)
            found.append(jnp.sum(high + low, axis=0, keepdims=True))
        return jnp.concatenate(found, axis=0)

    def scatter(g, values, base, depth):
        rows = row_of[pl.ds(pl.multiple_of(g * 8, 8), 8), :] - base
        high = values.astype(jnp.bfloat16).astype(jnp.float32)
        low = values - high
        row_iota = lax.broadcasted_iota(jnp.int32, (depth, LANES), 0)
        columns = []
        for i in range(8):
            hit = rows[i : i + 1, :] == row_iota
            upper = jnp.where(hit, high[i : i + 1, :], 0.0).astype(jnp.bfloat16)
            lower = jnp.where(hit, low[i : i + 1, :], 0.0).astype(jnp.bfloat16)
            columns.append(jnp.concatenate([upper, lower], axis=0))
        placed = jnp.concatenate(columns, axis=1)
        return lax.dot_general(
            placed, onehot[g], (((1,), (1,)), ((), ())), preferred_element_type=jnp.float32
        )

    def folded(both):
        depth = both.shape[0] // 2
        return both[0:depth] + both[depth : 2 * depth]

    def store(table, value):
        high, low = split(value)
        size = value.shape[0]
        table[0:size, :] = high
        table[size : 2 * size, :] = low

    def out_copy(turn, j):
        return pltpu.make_async_remote_copy(
            src_ref=out_src.at[turn, j],
            dst_ref=out_dst.at[turn, j],
            send_sem=out_send.at[turn, j],
            recv_sem=out_recv.at[turn, j],
            device_id=place(ring_peer(offsets[j])),
            device_id_type=MESH,
        )

    def back_copy(turn, j):
        return pltpu.make_async_remote_copy(
            src_ref=back_src.at[turn, j],
            dst_ref=back_dst.at[turn, j],
            send_sem=back_send.at[turn, j],
            recv_sem=back_recv.at[turn, j],
            device_id=place(ring_peer(-offsets[j])),
            device_id_type=MESH,
        )

    def near_copy(turn, step):
        return pltpu.make_async_remote_copy(
            src_ref=part.at[turn],
            dst_ref=first_buf.at[turn, near_id],
            send_sem=first_send.at[turn, step],
            recv_sem=first_recv.at[turn, step],
            device_id=place(near_peer(step)),
            device_id_type=MESH,
        )

    def far_copy(turn, step):
        return pltpu.make_async_remote_copy(
            src_ref=mid_part.at[turn],
            dst_ref=second_buf.at[turn, far_id],
            send_sem=second_send.at[turn, step],
            recv_sem=second_recv.at[turn, step],
            device_id=place(far_peer(step)),
            device_id_type=MESH,
        )

    def received(ref, turn, signs):
        rows = []
        for j in range(blocks):
            other = me + signs * offsets[j]
            inside = jnp.logical_and(other >= 0, other < count)
            rows.append(jnp.where(inside, ref[turn, j], 0.0))
        return jnp.concatenate(rows, axis=0)

    def group(g):
        return pl.ds(pl.multiple_of(g * 8, 8), 8)

    def apply(turn, vector, begin, middle):
        store(own_table, vector)
        per_group = 8 // block_rows
        for q in range(list_groups):
            found = gather(list_base + q, own_table, 0, own_rows)
            for r in range(per_group):
                j = q * per_group + r
                out_src[turn, j] = found[r * block_rows : (r + 1) * block_rows]
        if turn == 0:
            pl.semaphore_wait(barrier, len(peers))
        for j in range(blocks):
            out_copy(turn, j).start()

        def take_own(g, carry):
            cell_buf[group(g), :] = gather(g, own_table, 0, own_rows)
            return carry

        lax.fori_loop(0, cell_groups, take_own, 0, unroll=UNROLL)
        con_own = [gather(con_base + h, own_table, 0, own_rows) for h in range(con_rows)]
        for j in range(blocks):
            out_copy(turn, j).wait()
        ghosts = received(out_dst, turn, -1)
        padding = jnp.zeros((far_rows - ghost_rows, LANES), jnp.float32)
        store(ghost_table, jnp.concatenate([ghosts, padding], axis=0))
        resolved = []
        for h in range(con_rows):
            found = con_own[h] + gather(con_base + h, ghost_table, own_rows, ghost_rows)
            resolved.append(jnp.sum(weights[8 * h : 8 * h + 8, :] * found, axis=0, keepdims=True))
        resolved.append(jnp.zeros((far_rows - ghost_rows - con_rows, LANES), jnp.float32))
        store(ghost_table, jnp.concatenate([ghosts] + resolved, axis=0))

        def take_far(g, carry):
            cell_buf[group(g), :] += gather(g, ghost_table, own_rows, far_rows)
            return carry

        lax.fori_loop(0, cell_groups, take_far, 0, unroll=UNROLL)
        nodal = cell_buf[...]
        contrib = scale * jnp.dot(
            stiff_ref[...],
            nodal,
            precision=lax.Precision.HIGHEST,
            preferred_element_type=jnp.float32,
        )
        cell_buf[...] = contrib
        weighted = reaction_ref[...] * vector
        energy = jnp.sum(nodal * contrib, axis=0, keepdims=True)
        energy = energy + jnp.sum(weighted * vector, axis=0, keepdims=True)
        begin(energy)
        ghost_acc[...] = jnp.zeros_like(ghost_acc)

        def give_far(g, carry):
            ghost_acc[...] += scatter(g, cell_buf[group(g), :], own_rows, far_rows)
            return carry

        lax.fori_loop(0, cell_groups, give_far, 0, unroll=UNROLL)
        summed = folded(ghost_acc[...])
        spread = summed[0:ghost_rows]
        shares = []
        for h in range(con_rows):
            at = ghost_rows + h
            shares.append(weights[8 * h : 8 * h + 8, :] * summed[at : at + 1])
            spread = spread + folded(scatter(con_base + h, shares[h], own_rows, ghost_rows))
        for j in range(blocks):
            back_src[turn, j] = spread[j * block_rows : (j + 1) * block_rows]
        for j in range(blocks):
            back_copy(turn, j).start()
        middle()
        own_acc[...] = jnp.zeros_like(own_acc)

        def give_own(g, carry):
            own_acc[...] += scatter(g, cell_buf[group(g), :], 0, own_rows)
            return carry

        lax.fori_loop(0, cell_groups, give_own, 0, unroll=UNROLL)
        both = own_acc[...]
        for h in range(con_rows):
            both = both + scatter(con_base + h, shares[h], 0, own_rows)
        for j in range(blocks):
            back_copy(turn, j).wait()
        values = received(back_dst, turn, 1)
        for q in range(list_groups):
            both = both + scatter(list_base + q, values[8 * q : 8 * q + 8], 0, own_rows)
        return folded(both) + weighted

    def dot(one, two):
        return jnp.sum(one * two, axis=0, keepdims=True)

    def sums_start(turn, parts):
        mine = jnp.concatenate(parts, axis=0)
        part[turn] = mine
        first_buf[turn, near_id] = mine
        for step in range(1, near):
            near_copy(turn, step).start()

    def sums_middle(turn):
        for step in range(1, near):
            near_copy(turn, step).wait()
        mine = first_buf[turn, 0]
        for k in range(1, near):
            mine = mine + first_buf[turn, k]
        mid_part[turn] = mine
        second_buf[turn, far_id] = mine
        for step in range(1, far):
            far_copy(turn, step).start()

    def sums_end(turn):
        for step in range(1, far):
            far_copy(turn, step).wait()
        total = second_buf[turn, 0]
        for k in range(1, far):
            total = total + second_buf[turn, k]
        total = jnp.sum(total, axis=1, keepdims=True)
        return [total[k : k + 1] for k in range(SUMS)]

    start = right_ref[...]
    first = apply(0, start, lambda energy: None, lambda: None)
    known = [dot(start, start), dot(start, first), dot(first, first)]
    second = apply(
        1,
        first,
        lambda energy: sums_start(0, known + [energy]),
        lambda: sums_middle(0),
    )
    m0, m1, m2, m3 = sums_end(0)
    step0 = m0 / m1
    norm1 = m0 - 2.0 * step0 * m1 + step0 * step0 * m2
    product1 = m1 - 2.0 * step0 * m2 + step0 * step0 * m3
    ratio1 = norm1 / m0
    step1 = norm1 / (product1 - ratio1 * norm1 / step0)
    residual = start - step0 * first
    applied = first - step0 * second
    direction = residual + ratio1 * start
    applied_dir = applied + ratio1 * first
    answer = step0 * start + step1 * direction
    residual = residual - step1 * applied_dir
    zero = jnp.zeros((1, LANES), jnp.float32)
    square = dot(residual, residual)
    applied = apply(
        2,
        residual,
        lambda energy: sums_start(1, [square, energy, zero, zero]),
        lambda: sums_middle(1),
    )
    norm2, product2, unused_a, unused_b = sums_end(1)
    ratio2 = norm2 / norm1
    step2 = norm2 / (product2 - ratio2 * norm2 / step1)
    solution_ref[...] = answer + step2 * (residual + ratio2 * direction)
    residual_ref[...] = residual - step2 * (applied + ratio2 * applied_dir)


def on_device(shape, right_side, reaction, cell_slots, cell_level, con_masters, con_rows, send_lists):
    interp, stiffness = tables()
    own = right_side.shape[0]
    own_rows = own // LANES
    blocks, listed = send_lists.shape
    block_rows = listed // LANES
    con_tiles = con_rows.shape[0] // LANES
    points = cell_slots.shape[0]
    cell_rows = round_up(points, 8)
    far_rows = round_up(blocks * block_rows + con_tiles, 16)
    groups = cell_rows // 8 + blocks * block_rows // 8 + con_tiles
    padded = np.zeros((cell_rows, cell_rows), np.float32)
    padded[:points, :points] = stiffness
    count = shape[0] * shape[1]
    near = 1
    while near * near < count:
        near *= 2
    far = count // near
    operands = [
        right_side.reshape(own_rows, LANES),
        reaction.reshape(own_rows, LANES),
        cell_slots,
        cell_level.reshape(1, -1),
        con_masters,
        con_rows.reshape(con_tiles, LANES),
        send_lists,
        jnp.asarray(padded),
    ]
    exchange = pltpu.VMEM((ITERS, blocks, block_rows, LANES), jnp.float32)
    tile = jax.ShapeDtypeStruct((own_rows, LANES), jnp.float32)
    answer, residual = pl.pallas_call(
        functools.partial(kernel, shape, interp),
        out_shape=(tile, tile),
        in_specs=[pl.BlockSpec(memory_space=pl.ANY)] * 8,
        out_specs=(pl.BlockSpec(memory_space=pltpu.VMEM),) * 2,
        scratch_shapes=[
            *[pltpu.VMEM(value.shape, value.dtype) for value in operands],
            pltpu.SemaphoreType.DMA((len(operands),)),
            pltpu.VMEM((2 * own_rows, LANES), jnp.bfloat16),
            pltpu.VMEM((2 * far_rows, LANES), jnp.bfloat16),
            pltpu.VMEM((groups, LANES, 8 * LANES), jnp.bfloat16),
            pltpu.VMEM((groups * 8, LANES), jnp.int32),
            pltpu.VMEM((groups * 8, LANES), jnp.int32),
            pltpu.VMEM((con_tiles * 8, LANES), jnp.float32),
            pltpu.VMEM((cell_rows, LANES), jnp.float32),
            pltpu.VMEM((2 * own_rows, LANES), jnp.float32),
            pltpu.VMEM((2 * far_rows, LANES), jnp.float32),
            exchange,
            exchange,
            exchange,
            exchange,
            pltpu.VMEM((ROUNDS, SUMS, LANES), jnp.float32),
            pltpu.VMEM((ROUNDS, near, SUMS, LANES), jnp.float32),
            pltpu.VMEM((ROUNDS, SUMS, LANES), jnp.float32),
            pltpu.VMEM((ROUNDS, far, SUMS, LANES), jnp.float32),
            pltpu.SemaphoreType.DMA((ITERS, blocks)),
            pltpu.SemaphoreType.DMA((ITERS, blocks)),
            pltpu.SemaphoreType.DMA((ITERS, blocks)),
            pltpu.SemaphoreType.DMA((ITERS, blocks)),
            pltpu.SemaphoreType.DMA((ROUNDS, near)),
            pltpu.SemaphoreType.DMA((ROUNDS, near)),
            pltpu.SemaphoreType.DMA((ROUNDS, far)),
            pltpu.SemaphoreType.DMA((ROUNDS, far)),
        ],
        compiler_params=pltpu.CompilerParams(
            collective_id=0, has_side_effects=True, vmem_limit_bytes=60 * 1024 * 1024
        ),
    )(*operands)
    return (answer.reshape(own), residual.reshape(own))


def solution(mesh):
    placed = (
        P(("gx", "gy")),
        P(("gx", "gy")),
        P(None, ("gx", "gy")),
        P(("gx", "gy")),
        P(None, ("gx", "gy")),
        P(("gx", "gy")),
        P(None, ("gx", "gy")),
    )
    return jax.shard_map(
        functools.partial(on_device, (mesh.shape["gx"], mesh.shape["gy"])),
        mesh=mesh,
        in_specs=placed,
        out_specs=(P(("gx", "gy")), P(("gx", "gy"))),
        check_vma=False,
    )
```
